32 devices in a mesh: row: 4 (over y, x), col: 4 (over z), depth: 2 (over core).
Axes of the slice: x: 2, y: 2, z: 4, core: 2. Of those that a mesh axis runs over, the one named last changes fastest.
Arguments:
- layers: float32 [2, 4096, 4096], P('depth', 'row', 'col'), may hold values from -3 to 134.2, as said below
Outputs:
- factor: float32 [2, 4096, 512], P(None, 'row', 'depth')
- schur: float32 [4096, 4096], P(('row', 'depth'), 'col')
The draws below stay inside these ranges and needn't reach their ends.
Inputs may be any that keep to these rules, and one draw needn't show every extreme that they name: Read in matrix order, each layer is symmetric, and the sum over layers is symmetric positive definite with a diagonal of order sqrt(4096).
All inputs are finite; a program needn't handle non-finite values.
Results may differ from the reference program's by a relative error of at most 0.0001.
Values sent between devices are 32-bit elements; how exact they have to be, the bound alone decides.
A program may use at most 192 MiB of HBM per device.

```python
import jax
import jax.numpy as jnp
from jax import lax

PANEL = 512
BLOCKS_DEV = 2
PANELS = 2
LAYERS = 2
ORDER = 4096
COL_BLOCKS = 2
N_ROW = 4
N_COL = 4


def draw_layers(key, part):
    row_groups = ORDER // (PANEL * BLOCKS_DEV)
    col_groups = ORDER // (PANEL * COL_BLOCKS)
    positions = jnp.arange(ORDER, dtype=jnp.float32)
    distance = jnp.abs(positions[:, None] - positions[None, :])

    def one_layer(layer_index):
        layer_key = jax.random.fold_in(key, layer_index)
        noise_key, diag_key, scale_key, amp_key, reach_key = jax.random.split(layer_key, 5)
        noise = jnp.clip(jax.random.normal(noise_key, (ORDER, ORDER), jnp.float32), -4.0, 4.0)
        reach = PANEL * jax.random.uniform(reach_key, (), jnp.float32, 0.04, 0.12)
        amplitude = ORDER ** 0.5 * jax.random.uniform(amp_key, (), jnp.float32, 0.2, 0.45)
        symmetric = (noise + noise.T) * (0.5 / 1.4142135)
        row_scale = jax.random.uniform(scale_key, (ORDER,), jnp.float32, 0.7, 1.3)
        kernel = amplitude * row_scale[:, None] * row_scale[None, :] * jnp.exp(-distance / reach)
        diag_values = ORDER ** 0.5 * jax.random.uniform(diag_key, (ORDER,), jnp.float32, 0.75, 1.25)
        matrix = symmetric + kernel + jnp.diag(diag_values)
        rows = matrix.reshape(BLOCKS_DEV, row_groups, PANEL, ORDER).transpose(1, 0, 2, 3).reshape(ORDER, ORDER)
        return rows.reshape(ORDER, COL_BLOCKS, col_groups, PANEL).transpose(0, 2, 1, 3).reshape(ORDER, ORDER)
    return lax.map(one_layer, jnp.arange(LAYERS, dtype=jnp.int32)).astype(jnp.float32)


def setup_inputs(seed: int = 0) -> dict:
    streams_of = jax.random.split(jax.random.key(seed), 2)
    layers = draw_layers(jax.random.fold_in(streams_of[1], 71), 0)
    return dict(layers=layers)


def to_matrix(array):
    rows = array.reshape(N_ROW, BLOCKS_DEV, PANEL, ORDER).transpose(1, 0, 2, 3).reshape(ORDER, ORDER)
    return rows.reshape(ORDER, N_COL, COL_BLOCKS, PANEL).transpose(0, 2, 1, 3).reshape(ORDER, ORDER)

def rows_to_storage(matrix):
    width = matrix.shape[1]
    return matrix.reshape(BLOCKS_DEV, N_ROW, PANEL, width).transpose(1, 0, 2, 3).reshape(ORDER, width)

def to_storage(matrix):
    rows = rows_to_storage(matrix)
    return rows.reshape(ORDER, COL_BLOCKS, N_COL, PANEL).transpose(0, 2, 1, 3).reshape(ORDER, ORDER)

def reference(layers):
    matrix = to_matrix(jnp.sum(layers, axis=0))
    identity_block = jnp.eye(PANEL, dtype=jnp.float32)
    columns = []
    for panel_step in range(PANELS):
        first = panel_step * PANEL
        after = first + PANEL
        lower_diag = jnp.linalg.cholesky(matrix[first:after, first:after])
        inverse = jax.scipy.linalg.solve_triangular(lower_diag, identity_block, lower=True)
        solved = jnp.dot(matrix[first:, first:after], inverse.T, precision=lax.Precision.HIGHEST)
        column = jnp.concatenate([jnp.zeros((first, PANEL), jnp.float32), solved], axis=0)
        columns.append(rows_to_storage(column))
        below = solved[PANEL:]
        update = jnp.dot(below, below.T, precision=lax.Precision.HIGHEST)
        matrix = matrix.at[after:, after:].add(-update)
    return (jnp.stack(columns), to_storage(matrix))
```

```python
import functools

import jax
import jax.numpy as jnp
from jax import lax
from jax.experimental import pallas as pl
from jax.experimental.pallas import tpu as pltpu
from jax.sharding import PartitionSpec as P

PANEL = 512
PANELS = 2
INNER = 128
STRIP = 8
HIGH = lax.Precision.HIGH
HIGHEST = lax.Precision.HIGHEST


def dot(a, b, ca, cb, precision):
    return lax.dot_general(
        a, b, (((ca,), (cb,)), ((), ())), precision=precision, preferred_element_type=jnp.float32
    )


def tree(terms):
    while len(terms) > 1:
        terms = [terms[i] + terms[i + 1] if i + 1 < len(terms) else terms[i] for i in range(0, len(terms), 2)]
    return terms[0]

def factor_corner(work, inv):
    shape = (STRIP, INNER)
    sub = lax.broadcasted_iota(jnp.int32, shape, 0)
    lane = lax.broadcasted_iota(jnp.int32, shape, 1)
    def splat(x, t):
        return jnp.broadcast_to(x[t:t+1, :], shape)
    def column(x, j):
        return jnp.broadcast_to(x[:, j:j+1], shape)
    n = INNER // STRIP
    m = [work[a*STRIP:(a+1)*STRIP, :] for a in range(n)]
    for q in range(n):
        lo = q * STRIP
        panel = (lane >= lo) & (lane < lo + STRIP)
        rows = m[q]
        cols = [column(rows, lo + t) for t in range(STRIP)]
        full = jnp.where(panel, jnp.where(lane == lo + sub, 1.0, 0.0), rows)
        lower = full
        pivots = None
        for t in range(STRIP):
            pivot = splat(cols[t], t)
            pivots = pivot if pivots is None else jnp.where(sub >= t, pivot, pivots)
            scaled = cols[t] * (1.0 / pivot)
            both = jnp.where(sub == t, 0.0, scaled)
            for s in range(t + 1, STRIP):
                cols[s] = cols[s] - both * splat(cols[s], t)
            head = splat(full, t)
            full = full - both * head
            if t + 1 < STRIP:
                lower = lower - jnp.where(sub > t, scaled, 0.0) * head
        inv[lo:lo+STRIP, :] = jnp.where(lane < lo + STRIP, lower * lax.rsqrt(pivots), 0.0)
        if q + 1 < n:
            full = full * (1.0 / pivots)
            heads = [splat(full, t) for t in range(STRIP)]
            for a in range(q + 1, n):
                parts = tree([column(m[a], lo + t) * heads[t] for t in range(STRIP)])
                m[a] = jnp.where(panel, 0.0, m[a]) - parts

def inverse_kernel(block_ref, out_ref, whole, work, inv):
    size = block_ref.shape[0]
    whole[...] = block_ref[...]
    out_ref[...] = jnp.zeros_like(out_ref)
    def update(k):
        lo, hi = k * INNER, (k + 1) * INNER
        corner = inv[...]
        if k:
            out_ref[lo:hi, :lo] = dot(corner, out_ref[lo:hi, :lo], 1, 0, HIGHEST)
        out_ref[lo:hi, lo:hi] = corner
        if hi < size:
            below = dot(whole[hi:, lo:hi], corner, 1, 1, HIGHEST)
            whole[hi:, hi:] -= dot(below, below, 1, 1, HIGHEST)
            out_ref[hi:, :hi] -= dot(below, out_ref[lo:hi, :hi], 1, 0, HIGHEST)

    def step(k, carry):
        first = pl.ds(pl.multiple_of(k * INNER, INNER), INNER)
        work[...] = whole[first, first]
        factor_corner(work, inv)
        for static in range(size // INNER):
            pl.when(k == static)(functools.partial(update, static))
        return carry

    lax.fori_loop(0, size // INNER, step, 0)


def block_inverse(block):
    size = block.shape[0]
    return pl.pallas_call(
        inverse_kernel,
        out_shape=jax.ShapeDtypeStruct((size, size), jnp.float32),
        in_specs=[pl.BlockSpec(memory_space=pltpu.VMEM)],
        out_specs=pl.BlockSpec(memory_space=pltpu.VMEM),
        scratch_shapes=[
            pltpu.VMEM((size, size), jnp.float32),
            pltpu.VMEM((INNER, INNER), jnp.float32),
            pltpu.VMEM((INNER, INNER), jnp.float32),
        ],
        cost_estimate=pl.CostEstimate(flops=2 * size**3, bytes_accessed=8 * size**2, transcendentals=size),
        name="block_inverse",
    )(block)


def pick(index, table):
    value = 0
    for i, entry in enumerate(table):
        value = value + jnp.where(index == i, entry, 0)
    return value


def spread_kernel(groups, s_ref, rowp, colp, diag, zrecv, zsend, rrecv, rsend, srecv, ssend, lsem):
    row_groups, col_groups = groups
    r, c, d = lax.axis_index("row"), lax.axis_index("col"), lax.axis_index("depth")
    z_chunks, chunks = zrecv.shape[1], rrecv.shape[1]
    ring = list(range(row_groups))
    if row_groups & (row_groups - 1) == 0:
        ring = [i ^ (i >> 1) for i in ring]
    place = [ring.index(i) for i in range(row_groups)]
    pos = pick(r, place)
    after = pick(r, [ring[(place[i] + 1) % row_groups] for i in range(row_groups)])
    before = pick(r, [ring[(place[i] - 1) % row_groups] for i in range(row_groups)])
    target = jnp.where(d == 0, after, before)
    half = PANEL // 2
    last = []

    def local(src, dst):
        copy = pltpu.make_async_copy(src, dst, lsem)
        copy.start()
        copy.wait()

    def line(p, k):
        root, lane = p % col_groups, (p // col_groups) * PANEL
        size = PANEL // z_chunks
        rows = pl.ds(k * size, size)
        block = rowp.at[p, rows]

        def copy(way):
            return pltpu.make_async_remote_copy(
                src_ref=block,
                dst_ref=block,
                send_sem=zsend.at[p, k, max(way, 0)],
                recv_sem=zrecv.at[p, k],
                device_id={"col": c + way},
                device_id_type=pl.DeviceIdType.MESH,
            )

        @pl.when(c == root)
        def _():
            local(s_ref.at[rows, pl.ds(lane, PANEL)], block)

        @pl.when(c != root)
        def _():
            copy(1).wait_recv()

        up, down = (c >= root) & (c < col_groups - 1), (c <= root) & (c > 0)

        @pl.when(up)
        def _():
            copy(1).start()

        @pl.when(down)
        def _():
            copy(-1).start()

        def finish():
            @pl.when(up)
            def _():
                copy(1).wait_send()

            @pl.when(down)
            def _():
                copy(-1).wait_send()

        last.append(finish)

    def around(item, root, owner, src, dst, k):
        start = place[root]
        rel = jnp.where(d == 0, (pos - start + row_groups) % row_groups, (start - pos + row_groups) % row_groups)
        size = half // chunks
        own = pl.ds(pl.multiple_of(d * half + k * size, size), size)
        other = pl.ds(pl.multiple_of((1 - d) * half + k * size, size), size)
        is_root = rel == 0
        sends = rel < row_groups - 1
        origin = is_root & (d == owner)

        def hop():
            return pltpu.make_async_remote_copy(
                src_ref=dst.at[own],
                dst_ref=dst.at[own],
                send_sem=rsend.at[item, k],
                recv_sem=rrecv.at[item, k],
                device_id={"row": target},
                device_id_type=pl.DeviceIdType.MESH,
            )

        def across(kind):
            block = dst.at[(own, other)[kind]]
            return pltpu.make_async_remote_copy(
                src_ref=block,
                dst_ref=block,
                send_sem=ssend.at[item, kind, k],
                recv_sem=srecv.at[item, kind, k],
                device_id={"depth": 1 - d},
                device_id_type=pl.DeviceIdType.MESH,
            )

        @pl.when(origin)
        def _():
            local(src.at[other], dst.at[other])
            across(1).start()
            local(src.at[own], dst.at[own])
            across(0).start()

        @pl.when(is_root & (d != owner))
        def _():
            across(1).wait_recv()

        @pl.when(rel > 0)
        def _():
            hop().wait_recv()

        @pl.when(sends)
        def _():
            hop().start()

        @pl.when(rel > 0)
        def _():
            across(0).start()

        def finish():
            @pl.when(origin)
            def _():
                across(1).wait_send()
                across(0).wait_send()

            @pl.when(jnp.logical_not(origin))
            def _():
                across(0).wait_recv()

            @pl.when(rel > 0)
            def _():
                across(0).wait_send()

            @pl.when(sends)
            def _():
                hop().wait_send()

        last.append(finish)

    def owner_of(p):
        return p % row_groups, p // row_groups

    pairs = [(p, q) for p in range(PANELS) for q in range(p + 1)]
    order = [k for j in range(z_chunks // 2) for k in (j, j + z_chunks // 2)]
    for p in range(PANELS):
        for j in range(max(z_chunks, chunks)):
            if j < z_chunks:
                line(p, order[j])
            if j < chunks:
                around(len(pairs) + p, *owner_of(p), s_ref, colp.at[p], j)
        for item, (a, b) in enumerate(pairs):
            if b == p:
                for k in range(chunks):
                    around(item, *owner_of(a), rowp.at[b], diag.at[item], k)
    for finish in last:
        finish()


def spread(summed, row_groups, col_groups):
    cols = summed.shape[1]
    z_chunks, chunks = 8, 8
    blocks = PANELS * (PANELS + 1) // 2
    items = blocks + PANELS
    dma = pltpu.SemaphoreType.DMA
    vmem = pl.BlockSpec(memory_space=pltpu.VMEM)
    return pl.pallas_call(
        functools.partial(spread_kernel, (row_groups, col_groups)),
        out_shape=(
            jax.ShapeDtypeStruct((PANELS, PANEL, PANEL), jnp.float32),
            jax.ShapeDtypeStruct((PANELS, PANEL, cols), jnp.float32),
            jax.ShapeDtypeStruct((blocks, PANEL, PANEL), jnp.float32),
        ),
        in_specs=[vmem],
        out_specs=(vmem, vmem, vmem),
        scratch_shapes=[
            dma((PANELS, z_chunks)),
            dma((PANELS, z_chunks, 2)),
            dma((items, chunks)),
            dma((items, chunks)),
            dma((items, 2, chunks)),
            dma((items, 2, chunks)),
            dma,
        ],
        compiler_params=pltpu.CompilerParams(has_side_effects=True, vmem_limit_bytes=60 * 1024 * 1024),
        name="spread",
    )(summed)


def per_device(layers):
    row_groups = lax.axis_size("row")
    col_groups = lax.axis_size("col")
    depth_groups = lax.axis_size("depth")
    row = lax.axis_index("row")
    col = lax.axis_index("col")
    depth = lax.axis_index("depth")
    layer = layers[0]
    cols_local = layer.shape[1]
    assert layer.shape[0] == PANEL * depth_groups and depth_groups == 2

    swap = [(0, 1), (1, 0)]
    mine = lax.dynamic_slice_in_dim(layer, depth * PANEL, PANEL, 0)
    theirs = lax.dynamic_slice_in_dim(layer, (1 - depth) * PANEL, PANEL, 0)
    summed = mine + lax.ppermute(theirs, "depth", swap)
    own_block = row + row_groups * depth
    col_block = jnp.arange(cols_local, dtype=jnp.int32) // PANEL * col_groups + col

    rowp, colp, diag = spread(summed, row_groups, col_groups)
    rows = [rowp[p] for p in range(PANELS)]
    cols = [colp[p] for p in range(PANELS)]
    pairs = [(p, q) for p in range(PANELS) for q in range(p + 1)]
    lead = {pair: diag[i] for i, pair in enumerate(pairs)}
    factors, left, right = [], [], []
    for p in range(PANELS):
        inverse = block_inverse(lead[p, p])
        solved = {a: dot(lead[a, p], inverse, 1, 1, HIGHEST) for a in range(p + 1, PANELS)}
        for a in range(p + 1, PANELS):
            for b in range(p + 1, a + 1):
                lead[a, b] = lead[a, b] - dot(solved[a], solved[b], 1, 1, HIGHEST)
        c_rows = jnp.where(own_block >= p, dot(rows[p], inverse, 1, 1, HIGH), 0.0)
        below = jnp.where(own_block > p, c_rows, 0.0)
        c_cols = dot(inverse, cols[p], 1, 0, HIGH)
        c_cols = jnp.where((col_block > p)[None, :], c_cols, 0.0)
        factors.append(c_rows)
        left.append(below)
        right.append(c_cols)
        for q in range(p + 1, PANELS):
            rows[q] = rows[q] - dot(below, solved[q], 1, 1, HIGH)
            cols[q] = cols[q] - dot(solved[q], c_cols, 1, 0, HIGH)
    update = dot(jnp.concatenate(left, 1), jnp.concatenate(right, 0), 1, 0, HIGH)
    schur = summed - update
    factor = jnp.stack(factors)
    width = PANEL // depth_groups
    kept = lax.dynamic_slice_in_dim(factor, depth * width, width, 2)
    sent = lax.dynamic_slice_in_dim(factor, (1 - depth) * width, width, 2)
    got = lax.ppermute(sent, "depth", swap)
    first = jnp.where(depth == 0, kept, got)
    second = jnp.where(depth == 0, got, kept)
    return jnp.concatenate([first, second], axis=1), schur


def solution(mesh):
    return jax.shard_map(
        per_device,
        mesh=mesh,
        in_specs=(P("depth", "row", "col"),),
        out_specs=(P(None, "row", "depth"), P(("row", "depth"), "col")),
        check_vma=False,
    )
```

```python
import functools

import jax
import jax.numpy as jnp
from jax import lax
from jax.experimental import pallas as pl
from jax.experimental.pallas import tpu as pltpu
from jax.sharding import PartitionSpec as P

PANEL = 512
PANELS = 2
INNER = 128
STRIP = 8
STEPS = PANEL // INNER
TICKS = 4
CHUNKS = 8
LAG = 3
EARLY = 5
HIGH = lax.Precision.HIGH


def dot(a, b, ca, cb, precision=HIGH):
    return lax.dot_general(
        a, b, (((ca,), (cb,)), ((), ())), precision=precision, preferred_element_type=jnp.float32
    )


def tree(terms):
    while len(terms) > 1:
        terms = [terms[i] + terms[i + 1] if i + 1 < len(terms) else terms[i] for i in range(0, len(terms), 2)]
    return terms[0]


def factor_corner(work, inv, tick):
    shape = (STRIP, INNER)
    n = INNER // STRIP
    sub = lax.broadcasted_iota(jnp.int32, shape, 0)
    lane = lax.broadcasted_iota(jnp.int32, shape, 1)

    def splat(x, t):
        return jnp.broadcast_to(x[t : t + 1, :], shape)

    def column(x, j):
        return jnp.broadcast_to(x[:, j : j + 1], shape)

    def block(a):
        return slice(a * STRIP, (a + 1) * STRIP)

    m = None
    for q in range(n):
        if m is None:
            m = [work[block(a), :] for a in range(n)]
        lo = q * STRIP
        panel = (lane >= lo) & (lane < lo + STRIP)
        rows = m[q]
        cols = [column(rows, lo + t) for t in range(STRIP)]
        full = jnp.where(panel, jnp.where(lane == lo + sub, 1.0, 0.0), rows)
        lower = full
        pivots = None
        for t in range(STRIP):
            pivot = splat(cols[t], t)
            pivots = pivot if pivots is None else jnp.where(sub >= t, pivot, pivots)
            scaled = cols[t] * (1.0 / pivot)
            both = jnp.where(sub == t, 0.0, scaled)
            for s in range(t + 1, STRIP):
                cols[s] = cols[s] - both * splat(cols[s], t)
            head = splat(full, t)
            full = full - both * head
            if t + 1 < STRIP:
                lower = lower - jnp.where(sub > t, scaled, 0.0) * head
        inv[block(q), :] = jnp.where(lane < lo + STRIP, lower * lax.rsqrt(pivots), 0.0)
        if q + 1 < n:
            full = full * (1.0 / pivots)
            heads = [splat(full, t) for t in range(STRIP)]
            for a in range(q + 1, n):
                parts = tree([column(m[a], lo + t) * heads[t] for t in range(STRIP)])
                m[a] = jnp.where(panel, 0.0, m[a]) - parts
        if (q + 1) % 4 == 0:
            if q + 1 < n:
                for a in range(q + 1, n):
                    work[block(a), :] = m[a]
                m = None
            tick((q + 1) // 4 - 1)


def factor_block(source, inverse, lower, work, inv, held, pivot_block, tick, first):
    def before(k):
        lo, hi = k * INNER, (k + 1) * INNER
        block = source[lo:hi, lo:hi]
        if k:
            row = dot(source[lo:hi, :lo], inverse[:lo, :lo], 1, 1)
            block = block - dot(row, row, 1, 1)
            held[:, :lo] = dot(row, inverse[:lo, :lo], 1, 0)
            if lower is not None:
                lower[lo:hi, :lo] = row
        work[...] = block
        pivot_block[...] = block

    def after(k):
        lo, hi = k * INNER, (k + 1) * INNER
        corner = inv[...]
        if k:
            inverse[lo:hi, :lo] = -dot(corner, held[:, :lo], 1, 0)
        inverse[lo:hi, lo:hi] = corner
        if lower is not None:
            lower[lo:hi, lo:hi] = dot(pivot_block[...], corner, 1, 1)
        if hi < PANEL:
            inverse[lo:hi, hi:] = jnp.zeros((INNER, PANEL - hi), jnp.float32)
            if lower is not None:
                lower[lo:hi, hi:] = jnp.zeros((INNER, PANEL - hi), jnp.float32)

    def step(k, carry):
        for static in range(STEPS):
            pl.when(k == static)(functools.partial(before, static))
        factor_corner(work, inv, lambda i: tick(k, i, first + TICKS * k + i))
        for static in range(STEPS):
            pl.when(k == static)(functools.partial(after, static))
        return carry

    lax.fori_loop(0, STEPS, step, 0)


def pick(index, table):
    value = 0
    for i, entry in enumerate(table):
        value = value + jnp.where(index == i, entry, 0)
    return value


def lead_kernel(
    groups, layer, s_ref, rowp, colp, inverse, lower, solved,
    theirs, diag, rest, work, inv, held, pivot_block,
    dsend, drecv, dlocal, asend, arecv, zsend, zrecv,
    bsend, brecv, bxsend, bxrecv, csend, crecv, cxsend, cxrecv, lsem,
):
    row_groups, col_groups = groups
    r, c, d = lax.axis_index("row"), lax.axis_index("col"), lax.axis_index("depth")
    ring = list(range(row_groups))
    if row_groups & (row_groups - 1) == 0:
        ring = [i ^ (i >> 1) for i in ring]
    place = [ring.index(i) for i in range(row_groups)]
    pos = pick(r, place)
    after = pick(r, [ring[(place[i] + 1) % row_groups] for i in range(row_groups)])
    before = pick(r, [ring[(place[i] - 1) % row_groups] for i in range(row_groups)])
    target = jnp.where(d == 0, after, before)
    half = PANEL // 2
    second = jnp.where(d == 0, 0, 1)

    def remote(src, dst, send, recv, device):
        return pltpu.make_async_remote_copy(
            src_ref=src, dst_ref=dst, send_sem=send, recv_sem=recv,
            device_id=device, device_id_type=pl.DeviceIdType.MESH,
        )

    def local(src, dst):
        copy = pltpu.make_async_copy(src, dst, lsem)
        copy.start()
        copy.wait()

    top = (r == 0) & (d == 0)
    origin0 = top & (c == 0)
    far = list(range(col_groups - 1, 0, -1))
    wide = list(range(row_groups - 1, 0, -1))

    def piece(ref, k):
        return ref.at[pl.ds(k * INNER, INNER), pl.ds(0, (k + 1) * INNER)]

    def direct(src, k, slot, device):
        return remote(piece(src, k), piece(diag, k), asend.at[k, slot], arecv.at[k], device)

    def planes(k, src, act):
        for i, other in enumerate(wide):
            act(direct(src, k, len(far) + i, {"row": other}))
        act(direct(src, k, len(far) + len(wide), {"depth": 1}))

    def launch(k):
        @pl.when(origin0)
        def _():
            for i, other in enumerate(far):
                direct(s_ref, k, i, {"col": other}).start()
            planes(k, s_ref, lambda copy: copy.start())
            local(piece(s_ref, k), piece(diag, k))

    def arrive(k):
        @pl.when(jnp.logical_not(origin0))
        def _():
            direct(diag, k, 0, {"depth": 1 - d}).wait_recv()

        @pl.when(top & (c > 0))
        def _():
            planes(k, diag, lambda copy: copy.start())

        @pl.when((r > 0) & (d == 0))
        def _():
            direct(diag, k, len(far) + len(wide), {"depth": 1}).start()

    def settle(k):
        @pl.when(origin0)
        def _():
            for i, other in enumerate(far):
                direct(s_ref, k, i, {"col": other}).wait_send()

        @pl.when(top)
        def _():
            planes(k, diag, lambda copy: copy.wait_send())

        @pl.when((r > 0) & (d == 0))
        def _():
            direct(diag, k, len(far) + len(wide), {"depth": 1}).wait_send()

    def line(p, k, way):
        size = PANEL // CHUNKS
        block = rowp.at[p, pl.ds(pl.multiple_of(k * size, size), size)]
        return remote(block, block, zsend.at[p, k, max(way, 0)], zrecv.at[p, k], {"col": c + way})

    def line_set(p):
        hop = jnp.where(c > p, c - p, p - c)
        up, down = (c >= p) & (c < col_groups - 1), (c <= p) & (c > 0)
        needed = jnp.logical_not((r == 0) & (d == 0)) if p == 0 else jnp.bool_(True)
        return hop, up, down, needed

    def stream(dst, size, root, sems, index, k):
        send, recv, xsend, xrecv = sems
        rel = jnp.where(d == 0, (pos - place[root] + row_groups) % row_groups, (place[root] - pos + row_groups) % row_groups)
        own, other = size

        def hop():
            block = dst.at[own]
            return remote(block, block, send.at[index, k], recv.at[index, k], {"row": target})

        def across(kind):
            block = dst.at[(own, other)[kind]]
            return remote(block, block, xsend.at[index, kind, k], xrecv.at[index, kind, k], {"depth": 1 - d})

        return rel, hop, across

    def inject(src, dst, size, root, sems, index, k):
        rel, hop, across = stream(dst, size, root, sems, index, k)
        own, other = size
        local(src.at[other], dst.at[other])
        across(1).start()
        local(src.at[own], dst.at[own])
        hop().start()
        across(0).start()

    def relay(dst, size, root, sems, index, k):
        rel, hop, across = stream(dst, size, root, sems, index, k)

        @pl.when(rel == 0)
        def _():
            across(1).wait_recv()

        @pl.when(rel > 0)
        def _():
            hop().wait_recv()

        @pl.when(rel < row_groups - 1)
        def _():
            hop().start()

        @pl.when(rel > 0)
        def _():
            across(0).start()

    def finish(dst, size, root, sems, index, k, arrived):
        rel, hop, across = stream(dst, size, root, sems, index, k)
        origin = (rel == 0) & (d == 0)
        if arrived:
            @pl.when(jnp.logical_not(origin))
            def _():
                across(0).wait_recv()
            return

        @pl.when(origin)
        def _():
            across(1).wait_send()

        @pl.when((rel > 0) | origin)
        def _():
            across(0).wait_send()

        @pl.when(rel < row_groups - 1)
        def _():
            hop().wait_send()

    bsems = (bsend, brecv, bxsend, bxrecv)
    csems = (csend, crecv, cxsend, cxrecv)

    def bsize(k):
        size = PANEL // CHUNKS // 2
        return (
            pl.ds(pl.multiple_of((2 * k + d) * size, size), size),
            pl.ds(pl.multiple_of((2 * k + 1 - d) * size, size), size),
        )

    def csize(k):
        size = half // CHUNKS
        return (
            pl.ds(pl.multiple_of(d * half + k * size, size), size),
            pl.ds(pl.multiple_of((1 - d) * half + k * size, size), size),
        )

    last = PANELS - 1
    blocks_args = lambda item, k: (rest.at[item], bsize(k), item, bsems, item, k)
    cols_args = lambda p, k: (colp.at[p], csize(k), p, csems, p, k)

    def tick(n):
        for p in reversed(range(PANELS)):
            hop, up, down, needed = line_set(p)
            k = n - (CHUNKS * (last - p) + CHUNKS * PANELS * d + LAG * hop)

            @pl.when((k >= 0) & (k < CHUNKS) & needed)
            def _():
                @pl.when(c == p)
                def _():
                    size = PANEL // CHUNKS
                    rows = pl.ds(pl.multiple_of(k * size, size), size)
                    local(s_ref.at[rows, pl.ds(0, PANEL)], rowp.at[p, rows])

                @pl.when(c != p)
                def _():
                    line(p, k, 1).wait_recv()

                @pl.when(up)
                def _():
                    line(p, k, 1).start()

                @pl.when(down)
                def _():
                    line(p, k, -1).start()

                if p == last:
                    for item in range(PANELS):
                        @pl.when((r == item) & (d == 0))
                        def _():
                            inject(rowp.at[last], *blocks_args(item, k))

        hop = jnp.where(c > last, c - last, last - c)
        for item in range(PANELS):
            rel = stream(*blocks_args(item, 0))[0]
            k = n - (LAG * hop + LAG * rel + second)

            @pl.when((k >= 0) & (k < CHUNKS) & ((rel > 0) | (d != 0)))
            def _():
                relay(*blocks_args(item, k))

        for p in range(PANELS):
            rel = stream(*cols_args(p, 0))[0]
            k = n - (CHUNKS * p + CHUNKS + 4 + LAG * rel + second)

            @pl.when((k >= 0) & (k < CHUNKS))
            def _():
                @pl.when((rel == 0) & (d == 0))
                def _():
                    inject(s_ref, *cols_args(p, k))

                @pl.when((rel > 0) | (d != 0))
                def _():
                    relay(*cols_args(p, k))

    def ticks(lo, hi):
        def step(n, carry):
            tick(n)
            return carry

        lax.fori_loop(lo, hi, step, 0)

    def exchange(k):
        rows = pl.ds(k * INNER, INNER)
        mine = layer.at[0, pl.ds(pl.multiple_of(d * PANEL + k * INNER, INNER), INNER)]
        other = layer.at[0, pl.ds(pl.multiple_of((1 - d) * PANEL + k * INNER, INNER), INNER)]
        copy = remote(other, theirs.at[rows], dsend.at[k], drecv.at[k], {"depth": 1 - d})
        return copy, pltpu.make_async_copy(mine, s_ref.at[rows], dlocal.at[k])

    for k in range(STEPS):
        for copy in exchange(k):
            copy.start()
    for k in range(STEPS):
        copy, mine = exchange(k)
        mine.wait()
        copy.wait_recv()

        def add(i, carry):
            rows = pl.ds(pl.multiple_of(k * INNER + i * 32, 32), 32)
            s_ref[rows, :] = s_ref[rows, :] + theirs[rows, :]
            return carry

        lax.fori_loop(0, INNER // 32, add, 0)
        launch(k)

    @pl.when(top)
    def _():
        arrive(0)

    ticks(0, EARLY)

    @pl.when(jnp.logical_not(top))
    def _():
        arrive(0)

    def side(k, i, n):
        tick(n)
        if i == 2:
            for static in range(STEPS - 1):
                @pl.when(k == static)
                def _():
                    arrive(static + 1)

    scratch = (work, inv, held, pivot_block)
    factor_block(diag, inverse.at[0], lower, *scratch, side, EARLY)
    base = EARLY + TICKS * STEPS
    reach = CHUNKS + LAG * max(last, col_groups - 1 - last) + LAG * (row_groups - 1) + 1
    resume = max(base, reach)
    ticks(base, resume)

    def landed(k, carry):
        for item in range(PANELS):
            finish(*blocks_args(item, k), True)
        return carry

    lax.fori_loop(0, CHUNKS, landed, 0)
    solved[...] = dot(inverse[0], rest[0], 1, 0)
    whole = theirs.at[:, pl.ds(0, PANEL)]
    whole[...] = rest[1] - dot(solved[...], solved[...], 0, 0)
    factor_block(whole, inverse.at[1], None, *scratch, lambda k, i, n: tick(n), resume)
    lines = 2 * PANELS * CHUNKS + LAG * max(col_groups - 1, last)
    rings = PANELS * CHUNKS + CHUNKS + 5 + LAG * (row_groups - 1)
    ticks(resume + TICKS * STEPS, max(lines, rings))

    def close(k, carry):
        for p in range(PANELS):
            hop, up, down, needed = line_set(p)
            for way, on in ((1, up), (-1, down)):
                @pl.when(on & needed)
                def _():
                    line(p, k, way).wait_send()
            finish(*blocks_args(p, k), False)
            finish(*cols_args(p, k), True)
            finish(*cols_args(p, k), False)
        return carry

    lax.fori_loop(0, CHUNKS, close, 0)
    for k in range(STEPS):
        settle(k)
        exchange(k)[0].wait_send()


def lead(layer, row_groups, col_groups):
    cols = layer.shape[2]
    dma = pltpu.SemaphoreType.DMA
    vmem = pl.BlockSpec(memory_space=pltpu.VMEM)
    f32 = lambda *shape: jax.ShapeDtypeStruct(shape, jnp.float32)
    buffer = lambda *shape: pltpu.VMEM(shape, jnp.float32)
    return pl.pallas_call(
        functools.partial(lead_kernel, (row_groups, col_groups)),
        out_shape=(
            f32(PANEL, cols),
            f32(PANELS, PANEL, PANEL),
            f32(PANELS, PANEL, cols),
            f32(PANELS, PANEL, PANEL),
            f32(PANEL, PANEL),
            f32(PANEL, PANEL),
        ),
        in_specs=[pl.BlockSpec(memory_space=pl.ANY)],
        out_specs=(vmem,) * 6,
        scratch_shapes=[
            buffer(PANEL, cols),
            buffer(PANEL, PANEL),
            buffer(PANELS, PANEL, PANEL),
            buffer(INNER, INNER),
            buffer(INNER, INNER),
            buffer(INNER, PANEL),
            buffer(INNER, INNER),
            dma((STEPS,)),
            dma((STEPS,)),
            dma((STEPS,)),
            dma((STEPS, row_groups + col_groups - 1)),
            dma((STEPS,)),
            dma((PANELS, CHUNKS, 2)),
            dma((PANELS, CHUNKS)),
        ]
        + 2 * [dma((PANELS, CHUNKS)), dma((PANELS, CHUNKS)), dma((PANELS, 2, CHUNKS)), dma((PANELS, 2, CHUNKS))]
        + [dma],
        compiler_params=pltpu.CompilerParams(has_side_effects=True, vmem_limit_bytes=60 * 1024 * 1024),
        name="lead",
    )(layer)


def per_device(layers):
    row_groups = lax.axis_size("row")
    col_groups = lax.axis_size("col")
    depth_groups = lax.axis_size("depth")
    row = lax.axis_index("row")
    col = lax.axis_index("col")
    depth = lax.axis_index("depth")
    cols_local = layers.shape[2]
    assert layers.shape[1] == PANEL * depth_groups and depth_groups == 2
    assert PANELS == 2 and row_groups >= PANELS and col_groups >= PANELS

    swap = [(0, 1), (1, 0)]
    own_block = row + row_groups * depth
    col_block = jnp.arange(cols_local, dtype=jnp.int32) // PANEL * col_groups + col

    summed, rowp, colp, inverse, lower, solved = lead(layers, row_groups, col_groups)
    rows = [rowp[p] for p in range(PANELS)]
    cols = [colp[p] for p in range(PANELS)]
    factors, left, right = [], [], []
    for p in range(PANELS):
        c_rows = jnp.where(own_block >= p, dot(rows[p], inverse[p], 1, 1), 0.0)
        if p == 0:
            c_rows = jnp.where(own_block == 0, lower, c_rows)
        below = jnp.where(own_block > p, c_rows, 0.0)
        c_cols = dot(inverse[p], cols[p], 1, 0)
        c_cols = jnp.where((col_block > p)[None, :], c_cols, 0.0)
        factors.append(c_rows)
        left.append(below)
        right.append(c_cols)
        for q in range(p + 1, PANELS):
            rows[q] = rows[q] - dot(below, solved, 1, 0)
            cols[q] = cols[q] - dot(solved, c_cols, 0, 0)
    update = dot(jnp.concatenate(left, 1), jnp.concatenate(right, 0), 1, 0)
    schur = summed - update
    factor = jnp.stack(factors)
    width = PANEL // depth_groups
    kept = lax.dynamic_slice_in_dim(factor, depth * width, width, 2)
    sent = lax.dynamic_slice_in_dim(factor, (1 - depth) * width, width, 2)
    got = lax.ppermute(sent, "depth", swap)
    first = jnp.where(depth == 0, kept, got)
    second = jnp.where(depth == 0, got, kept)
    return jnp.concatenate([first, second], axis=1), schur


def solution(mesh):
    return jax.shard_map(
        per_device,
        mesh=mesh,
        in_specs=(P("depth", "row", "col"),),
        out_specs=(P(None, "row", "depth"), P(("row", "depth"), "col")),
        check_vma=False,
    )
```

```python
import functools

import jax
import jax.numpy as jnp
from jax import lax
from jax.experimental import pallas as pl
from jax.experimental.pallas import tpu as pltpu
from jax.sharding import PartitionSpec as P

PANEL = 512
PANELS = 2
INNER = 128
STRIP = 8
STEPS = PANEL // INNER
TICKS = 4
CHUNKS = 8
LAG = 3
SLACK = 4
START = 8
EARLY = 7
HIGH = lax.Precision.HIGH


def dot(a, b, ca, cb, precision=HIGH):
    return lax.dot_general(
        a, b, (((ca,), (cb,)), ((), ())), precision=precision, preferred_element_type=jnp.float32
    )


def tree(terms):
    while len(terms) > 1:
        terms = [terms[i] + terms[i + 1] if i + 1 < len(terms) else terms[i] for i in range(0, len(terms), 2)]
    return terms[0]


def factor_corner(work, inv, tick):
    shape = (STRIP, INNER)
    n = INNER // STRIP
    sub = lax.broadcasted_iota(jnp.int32, shape, 0)
    lane = lax.broadcasted_iota(jnp.int32, shape, 1)

    def splat(x, t):
        return jnp.broadcast_to(x[t : t + 1, :], shape)

    def column(x, j):
        return jnp.broadcast_to(x[:, j : j + 1], shape)

    def block(a):
        return slice(a * STRIP, (a + 1) * STRIP)

    m = None
    for q in range(n):
        if m is None:
            m = [work[block(a), :] for a in range(n)]
        lo = q * STRIP
        panel = (lane >= lo) & (lane < lo + STRIP)
        rows = m[q]
        cols = [column(rows, lo + t) for t in range(STRIP)]
        full = jnp.where(panel, jnp.where(lane == lo + sub, 1.0, 0.0), rows)
        lower = full
        pivots = None
        for t in range(STRIP):
            pivot = splat(cols[t], t)
            pivots = pivot if pivots is None else jnp.where(sub >= t, pivot, pivots)
            scaled = cols[t] * (1.0 / pivot)
            both = jnp.where(sub == t, 0.0, scaled)
            for s in range(t + 1, STRIP):
                cols[s] = cols[s] - both * splat(cols[s], t)
            head = splat(full, t)
            full = full - both * head
            if t + 1 < STRIP:
                lower = lower - jnp.where(sub > t, scaled, 0.0) * head
        inv[block(q), :] = jnp.where(lane < lo + STRIP, lower * lax.rsqrt(pivots), 0.0)
        if q + 1 < n:
            full = full * (1.0 / pivots)
            heads = [splat(full, t) for t in range(STRIP)]
            for a in range(q + 1, n):
                parts = tree([column(m[a], lo + t) * heads[t] for t in range(STRIP)])
                m[a] = jnp.where(panel, 0.0, m[a]) - parts
        if (q + 1) % 4 == 0:
            if q + 1 < n:
                for a in range(q + 1, n):
                    work[block(a), :] = m[a]
                m = None
            tick((q + 1) // 4 - 1)


def factor_block(source, inverse, lower, work, inv, held, pivot_block, tick, first, extra=None):
    def before(k):
        lo, hi = k * INNER, (k + 1) * INNER
        block = source[lo:hi, lo:hi]
        if k:
            row = dot(source[lo:hi, :lo], inverse[:lo, :lo], 1, 1)
            block = block - dot(row, row, 1, 1)
            held[:, :lo] = dot(row, inverse[:lo, :lo], 1, 0)
            if lower is not None:
                lower[lo:hi, :lo] = row
        work[...] = block
        pivot_block[...] = block

    def after(k):
        lo, hi = k * INNER, (k + 1) * INNER
        corner = inv[...]
        if k:
            inverse[lo:hi, :lo] = -dot(corner, held[:, :lo], 1, 0)
        inverse[lo:hi, lo:hi] = corner
        if lower is not None:
            lower[lo:hi, lo:hi] = dot(pivot_block[...], corner, 1, 1)
        if hi < PANEL:
            inverse[lo:hi, hi:] = jnp.zeros((INNER, PANEL - hi), jnp.float32)
            if lower is not None:
                lower[lo:hi, hi:] = jnp.zeros((INNER, PANEL - hi), jnp.float32)

    def step(k, carry):
        for static in range(STEPS):
            pl.when(k == static)(functools.partial(before, static))
        factor_corner(work, inv, lambda i: tick(k, i, first + TICKS * k + i))
        for static in range(STEPS):
            pl.when(k == static)(functools.partial(after, static))
        if extra is not None:
            pl.when(k == extra[0])(extra[1])
        return carry

    lax.fori_loop(0, STEPS, step, 0)


def pick(index, table):
    value = 0
    for i, entry in enumerate(table):
        value = value + jnp.where(index == i, entry, 0)
    return value


def lead_kernel(
    groups, layer, s_ref, factor, left, ccols,
    rowp, colp, inverse, lower, solved, crow, theirs, diag, rest, work, inv, held, pivot_block,
    dsend, drecv, dlocal, asend, arecv, zsend, zrecv,
    bsend, brecv, bxsend, bxrecv, csend, crecv, cxsend, cxrecv, fsend, frecv, lsem,
):
    row_groups, col_groups = groups
    r, c, d = lax.axis_index("row"), lax.axis_index("col"), lax.axis_index("depth")
    ring = list(range(row_groups))
    if row_groups & (row_groups - 1) == 0:
        ring = [i ^ (i >> 1) for i in ring]
    place = [ring.index(i) for i in range(row_groups)]
    pos = pick(r, place)
    after = pick(r, [ring[(place[i] + 1) % row_groups] for i in range(row_groups)])
    before = pick(r, [ring[(place[i] - 1) % row_groups] for i in range(row_groups)])
    target = jnp.where(d == 0, after, before)
    half = PANEL // 2
    last = PANELS - 1
    second = jnp.where(d == 0, 0, 1)

    def remote(src, dst, send, recv, device):
        return pltpu.make_async_remote_copy(
            src_ref=src, dst_ref=dst, send_sem=send, recv_sem=recv,
            device_id=device, device_id_type=pl.DeviceIdType.MESH,
        )

    def local(src, dst):
        copy = pltpu.make_async_copy(src, dst, lsem)
        copy.start()
        copy.wait()

    top = (r == 0) & (d == 0)
    origin0 = top & (c == 0)
    far = list(range(max(col_groups - 2, 1), 0, -1))
    relays = top & (c == col_groups - 2) if col_groups > 2 else jnp.bool_(False)
    wide = list(range(row_groups - 1, 0, -1))

    def piece(ref, k):
        return ref.at[pl.ds(k * INNER, INNER), pl.ds(0, (k + 1) * INNER)]

    def direct(src, k, slot, device):
        return remote(piece(src, k), piece(diag, k), asend.at[k, slot], arecv.at[k], device)

    def planes(k, src, act):
        for i, other in enumerate(wide):
            act(direct(src, k, len(far) + i, {"row": other}))
        act(direct(src, k, len(far) + len(wide), {"depth": 1}))

    def launch(k):
        @pl.when(origin0)
        def _():
            for i, other in enumerate(far):
                direct(s_ref, k, i, {"col": other}).start()
            planes(k, s_ref, lambda copy: copy.start())
            local(piece(s_ref, k), piece(diag, k))

    def arrive(k):
        @pl.when(jnp.logical_not(origin0))
        def _():
            direct(diag, k, 0, {"depth": 1 - d}).wait_recv()

        @pl.when(relays)
        def _():
            direct(diag, k, 0, {"col": c + 1}).start()

        @pl.when(top & (c > 0))
        def _():
            planes(k, diag, lambda copy: copy.start())

        @pl.when((r > 0) & (d == 0))
        def _():
            direct(diag, k, len(far) + len(wide), {"depth": 1}).start()

    def settle(k):
        @pl.when(origin0)
        def _():
            for i, other in enumerate(far):
                direct(s_ref, k, i, {"col": other}).wait_send()

        @pl.when(relays)
        def _():
            direct(diag, k, 0, {"col": c + 1}).wait_send()

        @pl.when(top)
        def _():
            planes(k, diag, lambda copy: copy.wait_send())

        @pl.when((r > 0) & (d == 0))
        def _():
            direct(diag, k, len(far) + len(wide), {"depth": 1}).wait_send()

    def line(p, k, way):
        size = PANEL // CHUNKS
        block = rowp.at[p, pl.ds(pl.multiple_of(k * size, size), size)]
        return remote(block, block, zsend.at[p, k, max(way, 0)], zrecv.at[p, k], {"col": c + way})

    def line_set(p):
        hop = jnp.where(c > p, c - p, p - c)
        up, down = (c >= p) & (c < col_groups - 1), (c <= p) & (c > 0)
        lead = r < PANELS
        first = lead & (d == 0)
        stride = jnp.where(lead, 1, 2)
        begin = jnp.where(lead, CHUNKS * (1 + p), 2 * CHUNKS * p) + SLACK * hop
        needed = jnp.logical_not(first)
        if p == last:
            begin = jnp.where(first, LAG * hop, begin)
            needed = jnp.bool_(True)
        return begin, stride, up, down, needed

    def stream(dst, size, root, sems, index, k):
        send, recv, xsend, xrecv = sems
        rel = jnp.where(d == 0, (pos - place[root] + row_groups) % row_groups, (place[root] - pos + row_groups) % row_groups)
        own, other = size

        def hop():
            block = dst.at[own]
            return remote(block, block, send.at[index, k], recv.at[index, k], {"row": target})

        def across(kind):
            block = dst.at[(own, other)[kind]]
            return remote(block, block, xsend.at[index, kind, k], xrecv.at[index, kind, k], {"depth": 1 - d})

        return rel, hop, across

    def inject(src, dst, size, root, sems, index, k):
        rel, hop, across = stream(dst, size, root, sems, index, k)
        own, other = size
        local(src.at[other], dst.at[other])
        across(1).start()
        local(src.at[own], dst.at[own])
        hop().start()
        across(0).start()

    def relay(dst, size, root, sems, index, k):
        rel, hop, across = stream(dst, size, root, sems, index, k)

        @pl.when(rel == 0)
        def _():
            across(1).wait_recv()

        @pl.when(rel > 0)
        def _():
            hop().wait_recv()

        @pl.when(rel < row_groups - 1)
        def _():
            hop().start()

        @pl.when(rel > 0)
        def _():
            across(0).start()

    def finish(dst, size, root, sems, index, k, arrived):
        rel, hop, across = stream(dst, size, root, sems, index, k)
        origin = (rel == 0) & (d == 0)
        if arrived:
            @pl.when(jnp.logical_not(origin))
            def _():
                across(0).wait_recv()
            return

        @pl.when(origin)
        def _():
            across(1).wait_send()

        @pl.when((rel > 0) | origin)
        def _():
            across(0).wait_send()

        @pl.when(rel < row_groups - 1)
        def _():
            hop().wait_send()

    bsems = (bsend, brecv, bxsend, bxrecv)
    csems = (csend, crecv, cxsend, cxrecv)

    def bsize(k):
        size = PANEL // CHUNKS // 2
        return (
            pl.ds(pl.multiple_of((2 * k + d) * size, size), size),
            pl.ds(pl.multiple_of((2 * k + 1 - d) * size, size), size),
        )

    def csize(k):
        size = half // CHUNKS
        return (
            pl.ds(pl.multiple_of(d * half + k * size, size), size),
            pl.ds(pl.multiple_of((1 - d) * half + k * size, size), size),
        )

    blocks_args = lambda item, k: (rest.at[item], bsize(k), item, bsems, item, k)
    cols_args = lambda p, k: (colp.at[p], csize(k), p, csems, p, k)

    def tick(n):
        for p in reversed(range(PANELS)):
            begin, stride, up, down, needed = line_set(p)
            k = (n - begin) // stride

            @pl.when((n >= begin) & ((n - begin) % stride == 0) & (k < CHUNKS) & needed)
            def _():
                @pl.when(c == p)
                def _():
                    size = PANEL // CHUNKS
                    rows = pl.ds(pl.multiple_of(k * size, size), size)
                    local(s_ref.at[rows, pl.ds(0, PANEL)], rowp.at[p, rows])

                @pl.when(c != p)
                def _():
                    line(p, k, 1).wait_recv()

                @pl.when(up)
                def _():
                    line(p, k, 1).start()

                @pl.when(down)
                def _():
                    line(p, k, -1).start()

                if p == last:
                    for item in range(PANELS):
                        @pl.when((r == item) & (d == 0))
                        def _():
                            inject(rowp.at[last], *blocks_args(item, k))

        hop = jnp.where(c > last, c - last, last - c)
        for item in range(PANELS):
            rel = stream(*blocks_args(item, 0))[0]
            k = n - (LAG * hop + LAG * rel + second)

            @pl.when((k >= 0) & (k < CHUNKS) & ((rel > 0) | (d != 0)))
            def _():
                relay(*blocks_args(item, k))

        for p in range(PANELS):
            rel = stream(*cols_args(p, 0))[0]
            k = n - (START + CHUNKS * p + SLACK * rel + second)

            @pl.when((k >= 0) & (k < CHUNKS))
            def _():
                @pl.when((rel == 0) & (d == 0))
                def _():
                    inject(s_ref, *cols_args(p, k))

                @pl.when((rel > 0) | (d != 0))
                def _():
                    relay(*cols_args(p, k))

    def ticks(lo, hi):
        def step(n, carry):
            tick(n)
            return carry

        lax.fori_loop(lo, hi, step, 0)

    def exchange(k):
        rows = pl.ds(k * INNER, INNER)
        mine = layer.at[0, pl.ds(pl.multiple_of(d * PANEL + k * INNER, INNER), INNER)]
        other = layer.at[0, pl.ds(pl.multiple_of((1 - d) * PANEL + k * INNER, INNER), INNER)]
        copy = remote(other, theirs.at[rows], dsend.at[k], drecv.at[k], {"depth": 1 - d})
        return copy, pltpu.make_async_copy(mine, s_ref.at[rows], dlocal.at[k])

    for k in range(STEPS):
        for copy in exchange(k):
            copy.start()
    for k in range(STEPS):
        copy, mine = exchange(k)
        mine.wait()
        copy.wait_recv()

        def add(i, carry):
            rows = pl.ds(pl.multiple_of(k * INNER + i * 32, 32), 32)
            s_ref[rows, :] = s_ref[rows, :] + theirs[rows, :]
            return carry

        lax.fori_loop(0, INNER // 32, add, 0)
        launch(k)

    @pl.when(top)
    def _():
        arrive(0)

    ticks(0, EARLY)

    @pl.when(jnp.logical_not(top))
    def _():
        arrive(0)

    other = jnp.logical_not(top)
    plan = [(0, 1, top), (2, 2, top), (6, 3, top), (2, 1, other), (6, 2, other), (10, 3, other)]

    def side(k, i, n):
        tick(n)
        for at, piece_index, who in plan:
            if i == at % TICKS:
                @pl.when((k == at // TICKS) & who)
                def _():
                    arrive(piece_index)

    scratch = (work, inv, held, pivot_block)
    factor_block(diag, inverse.at[0], lower, *scratch, side, EARLY)
    base = EARLY + TICKS * STEPS
    reach = CHUNKS + LAG * max(last, col_groups - 1 - last) + LAG * (row_groups - 1) + 1
    resume = max(base, reach)
    ticks(base, resume)

    def landed(k, carry):
        for item in range(PANELS):
            finish(*blocks_args(item, k), True)
        return carry

    lax.fori_loop(0, CHUNKS, landed, 0)
    solved[...] = dot(inverse[0], rest[0], 1, 0)

    @pl.when((r == 1) & (d == 0))
    def _():
        lower[...] = solved[...].T

    whole = theirs.at[:, pl.ds(0, PANEL)]
    whole[...] = rest[1] - dot(solved[...], solved[...], 0, 0)
    for k in range(STEPS):
        settle(k)
        exchange(k)[0].wait_send()

    own_block = r + row_groups * d

    def tiles(count, size, body):
        def step(t, carry):
            body(pl.ds(pl.multiple_of(t * size, size), size), t)
            return carry

        lax.fori_loop(0, count // size, step, 0)

    def live(t, p):
        return t * col_groups + c > p

    def first_rows(lanes, t):
        value = jnp.where(own_block < PANELS, lower[:, lanes], dot(rowp[0], inverse[0, lanes, :], 1, 1))
        crow[0, :, lanes] = value
        left[:, lanes] = jnp.where(own_block > 0, value, 0.0)

    def first_cols(lanes, t):
        value = jnp.where(live(t, 0), dot(inverse[0], colp[0, :, lanes], 1, 0), 0.0)
        ccols[:, lanes] = value
        s_ref[:, lanes] = s_ref[:, lanes] - dot(left[...], value, 1, 0)

    def between_rows(lanes, t):
        rowp[1, :, lanes] = rowp[1, :, lanes] - dot(left[...], solved[:, lanes], 1, 0)

    def second_rows(lanes, t):
        value = jnp.where(own_block > 0, dot(rowp[1], inverse[1, lanes, :], 1, 1), 0.0)
        crow[1, :, lanes] = value
        left[:, lanes] = jnp.where(own_block > 1, value, 0.0)

    def second_cols(lanes, t):
        value = colp[1, :, lanes] - dot(solved[...], ccols[:, lanes], 0, 0)
        value = dot(inverse[1], value, 1, 0)
        value = jnp.where(live(t, 1), value, 0.0)
        s_ref[:, lanes] = s_ref[:, lanes] - dot(left[...], value, 1, 0)

    def arrived_cols(p):
        def step(k, carry):
            finish(*cols_args(p, k), True)
            return carry

        lax.fori_loop(0, CHUNKS, step, 0)

    def give(p):
        sent = crow.at[p, :, pl.ds(pl.multiple_of((1 - d) * half, half), half)]
        there = factor.at[p, pl.ds(pl.multiple_of(d * PANEL, PANEL), PANEL), :]
        return remote(sent, there, fsend.at[p], frecv.at[p], {"depth": 1 - d})

    def keep(p):
        kept = crow[p, :, pl.ds(pl.multiple_of(d * half, half), half)]
        factor[p, pl.ds(pl.multiple_of(d * PANEL, PANEL), PANEL), :] = kept

    def first_panel():
        tiles(PANEL, half, first_rows)
        arrived_cols(0)
        tiles(s_ref.shape[1], PANEL, first_cols)
        keep(0)
        give(0).start()

    lines = 2 * PANELS * CHUNKS + SLACK * max(col_groups - 1, last)
    rings = PANELS * CHUNKS + START + 1 + SLACK * (row_groups - 1)
    ready = max(lines - CHUNKS * PANELS, rings - CHUNKS, 2 * CHUNKS * PANELS)
    early = -(-(ready - resume) // TICKS) - 1
    extra = (early, first_panel) if early < STEPS else None
    factor_block(whole, inverse.at[1], None, *scratch, lambda k, i, n: tick(n), resume, extra)
    ticks(resume + TICKS * STEPS, max(lines, rings))
    if extra is None:
        first_panel()

    def close(k, carry):
        for p in range(PANELS):
            begin, stride, up, down, needed = line_set(p)
            for way, on in ((1, up), (-1, down)):
                @pl.when(on & needed)
                def _():
                    line(p, k, way).wait_send()
            finish(*blocks_args(p, k), False)
            finish(*cols_args(p, k), False)
        return carry

    lax.fori_loop(0, CHUNKS, close, 0)
    arrived_cols(1)
    tiles(PANEL, half, between_rows)
    tiles(PANEL, half, second_rows)
    keep(1)
    give(1).start()
    tiles(s_ref.shape[1], PANEL, second_cols)
    for p in range(PANELS):
        give(p).wait()


def lead(layer, row_groups, col_groups):
    cols = layer.shape[2]
    dma = pltpu.SemaphoreType.DMA
    vmem = pl.BlockSpec(memory_space=pltpu.VMEM)
    f32 = lambda *shape: jax.ShapeDtypeStruct(shape, jnp.float32)
    buffer = lambda *shape: pltpu.VMEM(shape, jnp.float32)
    return pl.pallas_call(
        functools.partial(lead_kernel, (row_groups, col_groups)),
        out_shape=(
            f32(PANEL, cols),
            f32(PANELS, 2 * PANEL, PANEL // 2),
        ),
        in_specs=[pl.BlockSpec(memory_space=pl.ANY)],
        out_specs=(vmem,) * 2,
        scratch_shapes=[
            buffer(PANEL, PANEL),
            buffer(PANEL, cols),
            buffer(PANELS, PANEL, PANEL),
            buffer(PANELS, PANEL, cols),
            buffer(PANELS, PANEL, PANEL),
            buffer(PANEL, PANEL),
            buffer(PANEL, PANEL),
            buffer(PANELS, PANEL, PANEL),
            buffer(PANEL, cols),
            buffer(PANEL, PANEL),
            buffer(PANELS, PANEL, PANEL),
            buffer(INNER, INNER),
            buffer(INNER, INNER),
            buffer(INNER, PANEL),
            buffer(INNER, INNER),
            dma((STEPS,)),
            dma((STEPS,)),
            dma((STEPS,)),
            dma((STEPS, row_groups + col_groups - 1)),
            dma((STEPS,)),
            dma((PANELS, CHUNKS, 2)),
            dma((PANELS, CHUNKS)),
        ]
        + 2 * [dma((PANELS, CHUNKS)), dma((PANELS, CHUNKS)), dma((PANELS, 2, CHUNKS)), dma((PANELS, 2, CHUNKS))]
        + [dma((PANELS,)), dma((PANELS,)), dma],
        compiler_params=pltpu.CompilerParams(has_side_effects=True, vmem_limit_bytes=60 * 1024 * 1024),
        name="lead",
    )(layer)


def per_device(layers):
    row_groups = lax.axis_size("row")
    col_groups = lax.axis_size("col")
    depth_groups = lax.axis_size("depth")
    assert layers.shape[1] == PANEL * depth_groups and depth_groups == 2
    assert PANELS == 2 and row_groups >= PANELS and col_groups >= PANELS

    schur, factor = lead(layers, row_groups, col_groups)
    return factor, schur


def solution(mesh):
    return jax.shard_map(
        per_device,
        mesh=mesh,
        in_specs=(P("depth", "row", "col"),),
        out_specs=(P(None, "row", "depth"), P(("row", "depth"), "col")),
        check_vma=False,
    )
```

```python
import functools

import jax
import jax.numpy as jnp
from jax import lax
from jax.experimental import pallas as pl
from jax.experimental.pallas import tpu as pltpu
from jax.sharding import PartitionSpec as P

PANEL = 512
PANELS = 2
INNER = 128
STRIP = 8
STEPS = PANEL // INNER
TICKS = 4
CHUNKS = 8
LAG = 3
SLACK = 4
START = 8
EARLY = 7
HIGH = lax.Precision.HIGH


def dot(a, b, ca, cb, precision=HIGH):
    return lax.dot_general(
        a, b, (((ca,), (cb,)), ((), ())), precision=precision, preferred_element_type=jnp.float32
    )


def tree(terms):
    while len(terms) > 1:
        terms = [terms[i] + terms[i + 1] if i + 1 < len(terms) else terms[i] for i in range(0, len(terms), 2)]
    return terms[0]


def factor_corner(work, inv, tick):
    shape = (STRIP, INNER)
    n = INNER // STRIP
    sub = lax.broadcasted_iota(jnp.int32, shape, 0)
    lane = lax.broadcasted_iota(jnp.int32, shape, 1)

    def splat(x, t):
        return jnp.broadcast_to(x[t : t + 1, :], shape)

    def column(x, j):
        return jnp.broadcast_to(x[:, j : j + 1], shape)

    def block(a):
        return slice(a * STRIP, (a + 1) * STRIP)

    m = None
    for q in range(n):
        if m is None:
            m = [work[block(a), :] for a in range(n)]
        lo = q * STRIP
        panel = (lane >= lo) & (lane < lo + STRIP)
        rows = m[q]
        cols = [column(rows, lo + t) for t in range(STRIP)]
        full = jnp.where(panel, jnp.where(lane == lo + sub, 1.0, 0.0), rows)
        lower = full
        pivots = None
        for t in range(STRIP):
            pivot = splat(cols[t], t)
            pivots = pivot if pivots is None else jnp.where(sub >= t, pivot, pivots)
            scaled = cols[t] * (1.0 / pivot)
            both = jnp.where(sub == t, 0.0, scaled)
            for s in range(t + 1, STRIP):
                cols[s] = cols[s] - both * splat(cols[s], t)
            head = splat(full, t)
            full = full - both * head
            if t + 1 < STRIP:
                lower = lower - jnp.where(sub > t, scaled, 0.0) * head
        inv[block(q), :] = jnp.where(lane < lo + STRIP, lower * lax.rsqrt(pivots), 0.0)
        if q + 1 < n:
            full = full * (1.0 / pivots)
            heads = [splat(full, t) for t in range(STRIP)]
            for a in range(q + 1, n):
                parts = tree([column(m[a], lo + t) * heads[t] for t in range(STRIP)])
                m[a] = jnp.where(panel, 0.0, m[a]) - parts
        if (q + 1) % 4 == 0:
            if q + 1 < n:
                for a in range(q + 1, n):
                    work[block(a), :] = m[a]
                m = None
            tick((q + 1) // 4 - 1)


def factor_block(source, inverse, lower, work, inv, held, pivot_block, tick, first, extra=None):
    def before(k):
        lo, hi = k * INNER, (k + 1) * INNER
        block = source[lo:hi, lo:hi]
        if k:
            row = dot(source[lo:hi, :lo], inverse[:lo, :lo], 1, 1)
            block = block - dot(row, row, 1, 1)
            held[:, :lo] = dot(row, inverse[:lo, :lo], 1, 0)
            if lower is not None:
                lower[lo:hi, :lo] = row
        work[...] = block
        pivot_block[...] = block

    def after(k):
        lo, hi = k * INNER, (k + 1) * INNER
        corner = inv[...]
        if k:
            inverse[lo:hi, :lo] = -dot(corner, held[:, :lo], 1, 0)
        inverse[lo:hi, lo:hi] = corner
        if lower is not None:
            lower[lo:hi, lo:hi] = dot(pivot_block[...], corner, 1, 1)
        if hi < PANEL:
            inverse[lo:hi, hi:] = jnp.zeros((INNER, PANEL - hi), jnp.float32)
            if lower is not None:
                lower[lo:hi, hi:] = jnp.zeros((INNER, PANEL - hi), jnp.float32)

    def step(k, carry):
        for static in range(STEPS):
            pl.when(k == static)(functools.partial(before, static))
        factor_corner(work, inv, lambda i: tick(k, i, first + TICKS * k + i))
        for static in range(STEPS):
            pl.when(k == static)(functools.partial(after, static))
        if extra is not None:
            pl.when(k == extra[0])(extra[1])
        return carry

    lax.fori_loop(0, STEPS, step, 0)


def pick(index, table):
    value = 0
    for i, entry in enumerate(table):
        value = value + jnp.where(index == i, entry, 0)
    return value


def lead_kernel(
    groups, layer, s_ref, factor, left, ccols,
    rowp, colp, inverse, lower, solved, crow, theirs, diag, rest, work, inv, held, pivot_block,
    dsend, drecv, dlocal, asend, arecv, zsend, zrecv,
    bsend, brecv, bxsend, bxrecv, csend, crecv, cxsend, cxrecv, fsend, frecv, lsem,
):
    row_groups, col_groups = groups
    r, c, d = lax.axis_index("row"), lax.axis_index("col"), lax.axis_index("depth")
    ring = list(range(row_groups))
    if row_groups & (row_groups - 1) == 0:
        ring = [i ^ (i >> 1) for i in ring]
    place = [ring.index(i) for i in range(row_groups)]
    pos = pick(r, place)
    after = pick(r, [ring[(place[i] + 1) % row_groups] for i in range(row_groups)])
    before = pick(r, [ring[(place[i] - 1) % row_groups] for i in range(row_groups)])
    target = jnp.where(d == 0, after, before)
    half = PANEL // 2
    last = PANELS - 1
    second = jnp.where(d == 0, 0, 1)

    def remote(src, dst, send, recv, device):
        return pltpu.make_async_remote_copy(
            src_ref=src, dst_ref=dst, send_sem=send, recv_sem=recv,
            device_id=device, device_id_type=pl.DeviceIdType.MESH,
        )

    def local(src, dst):
        copy = pltpu.make_async_copy(src, dst, lsem)
        copy.start()
        copy.wait()

    top = (r == 0) & (d == 0)
    origin0 = top & (c == 0)
    far = list(range(max(col_groups - 2, 1), 0, -1))
    relays = top & (c == col_groups - 2) if col_groups > 2 else jnp.bool_(False)
    wide = list(range(row_groups - 1, 0, -1))

    def piece(ref, k):
        return ref.at[pl.ds(k * INNER, INNER), pl.ds(0, (k + 1) * INNER)]

    def direct(src, k, slot, device):
        return remote(piece(src, k), piece(diag, k), asend.at[k, slot], arecv.at[k], device)

    def planes(k, src, act):
        for i, other in enumerate(wide):
            act(direct(src, k, len(far) + i, {"row": other}))
        act(direct(src, k, len(far) + len(wide), {"depth": 1}))

    def launch(k):
        @pl.when(origin0)
        def _():
            for i, other in enumerate(far):
                direct(s_ref, k, i, {"col": other}).start()
            planes(k, s_ref, lambda copy: copy.start())
            local(piece(s_ref, k), piece(diag, k))

    def arrive(k):
        @pl.when(jnp.logical_not(origin0))
        def _():
            direct(diag, k, 0, {"depth": 1 - d}).wait_recv()

        @pl.when(relays)
        def _():
            direct(diag, k, 0, {"col": c + 1}).start()

        @pl.when(top & (c > 0))
        def _():
            planes(k, diag, lambda copy: copy.start())

        @pl.when((r > 0) & (d == 0))
        def _():
            direct(diag, k, len(far) + len(wide), {"depth": 1}).start()

    def settle(k):
        @pl.when(origin0)
        def _():
            for i, other in enumerate(far):
                direct(s_ref, k, i, {"col": other}).wait_send()

        @pl.when(relays)
        def _():
            direct(diag, k, 0, {"col": c + 1}).wait_send()

        @pl.when(top)
        def _():
            planes(k, diag, lambda copy: copy.wait_send())

        @pl.when((r > 0) & (d == 0))
        def _():
            direct(diag, k, len(far) + len(wide), {"depth": 1}).wait_send()

    def line(p, k, way):
        size = PANEL // CHUNKS
        block = rowp.at[p, pl.ds(pl.multiple_of(k * size, size), size)]
        return remote(block, block, zsend.at[p, k, max(way, 0)], zrecv.at[p, k], {"col": c + way})

    def line_set(p):
        hop = jnp.where(c > p, c - p, p - c)
        up, down = (c >= p) & (c < col_groups - 1), (c <= p) & (c > 0)
        lead = r < PANELS
        first = lead & (d == 0)
        stride = jnp.where(lead, 1, 2)
        begin = jnp.where(lead, CHUNKS * (1 + p), 2 * CHUNKS * p) + SLACK * hop
        needed = jnp.logical_not(first)
        if p == last:
            begin = jnp.where(first, LAG * hop, begin)
            needed = jnp.bool_(True)
        return begin, stride, up, down, needed

    def stream(dst, size, root, sems, index, k):
        send, recv, xsend, xrecv = sems
        rel = jnp.where(d == 0, (pos - place[root] + row_groups) % row_groups, (place[root] - pos + row_groups) % row_groups)
        own, other = size

        def hop():
            block = dst.at[own]
            return remote(block, block, send.at[index, k], recv.at[index, k], {"row": target})

        def across(kind):
            block = dst.at[(own, other)[kind]]
            return remote(block, block, xsend.at[index, kind, k], xrecv.at[index, kind, k], {"depth": 1 - d})

        return rel, hop, across

    def inject(src, dst, size, root, sems, index, k):
        rel, hop, across = stream(dst, size, root, sems, index, k)
        own, other = size
        local(src.at[other], dst.at[other])
        across(1).start()
        local(src.at[own], dst.at[own])
        hop().start()
        across(0).start()

    def relay(dst, size, root, sems, index, k):
        rel, hop, across = stream(dst, size, root, sems, index, k)

        @pl.when(rel == 0)
        def _():
            across(1).wait_recv()

        @pl.when(rel > 0)
        def _():
            hop().wait_recv()

        @pl.when(rel < row_groups - 1)
        def _():
            hop().start()

        @pl.when(rel > 0)
        def _():
            across(0).start()

    def finish(dst, size, root, sems, index, k, arrived):
        rel, hop, across = stream(dst, size, root, sems, index, k)
        origin = (rel == 0) & (d == 0)
        if arrived:
            @pl.when(jnp.logical_not(origin))
            def _():
                across(0).wait_recv()
            return

        @pl.when(origin)
        def _():
            across(1).wait_send()

        @pl.when((rel > 0) | origin)
        def _():
            across(0).wait_send()

        @pl.when(rel < row_groups - 1)
        def _():
            hop().wait_send()

    bsems = (bsend, brecv, bxsend, bxrecv)
    csems = (csend, crecv, cxsend, cxrecv)

    def bsize(k):
        size = PANEL // CHUNKS // 2
        return (
            pl.ds(pl.multiple_of((2 * k + d) * size, size), size),
            pl.ds(pl.multiple_of((2 * k + 1 - d) * size, size), size),
        )

    def csize(k):
        size = half // CHUNKS
        return (
            pl.ds(pl.multiple_of(d * half + k * size, size), size),
            pl.ds(pl.multiple_of((1 - d) * half + k * size, size), size),
        )

    blocks_args = lambda item, k: (rest.at[item], bsize(k), item, bsems, item, k)
    cols_args = lambda p, k: (colp.at[p], csize(k), p, csems, p, k)

    def tick(n):
        for p in reversed(range(PANELS)):
            begin, stride, up, down, needed = line_set(p)
            k = (n - begin) // stride

            @pl.when((n >= begin) & ((n - begin) % stride == 0) & (k < CHUNKS) & needed)
            def _():
                @pl.when(c == p)
                def _():
                    size = PANEL // CHUNKS
                    rows = pl.ds(pl.multiple_of(k * size, size), size)
                    local(s_ref.at[rows, pl.ds(0, PANEL)], rowp.at[p, rows])

                @pl.when(c != p)
                def _():
                    line(p, k, 1).wait_recv()

                @pl.when(up)
                def _():
                    line(p, k, 1).start()

                @pl.when(down)
                def _():
                    line(p, k, -1).start()

                if p == last:
                    for item in range(PANELS):
                        @pl.when((r == item) & (d == 0))
                        def _():
                            inject(rowp.at[last], *blocks_args(item, k))

        hop = jnp.where(c > last, c - last, last - c)
        for item in range(PANELS):
            rel = stream(*blocks_args(item, 0))[0]
            k = n - (LAG * hop + LAG * rel + second)

            @pl.when((k >= 0) & (k < CHUNKS) & ((rel > 0) | (d != 0)))
            def _():
                relay(*blocks_args(item, k))

        for p in range(PANELS):
            rel = stream(*cols_args(p, 0))[0]
            k = n - (START + CHUNKS * p + SLACK * rel + second)

            @pl.when((k >= 0) & (k < CHUNKS))
            def _():
                @pl.when((rel == 0) & (d == 0))
                def _():
                    inject(s_ref, *cols_args(p, k))

                @pl.when((rel > 0) | (d != 0))
                def _():
                    relay(*cols_args(p, k))

    def ticks(lo, hi):
        def step(n, carry):
            tick(n)
            return carry

        lax.fori_loop(lo, hi, step, 0)

    def exchange(k):
        rows = pl.ds(k * INNER, INNER)
        mine = layer.at[0, pl.ds(pl.multiple_of(d * PANEL + k * INNER, INNER), INNER)]
        other = layer.at[0, pl.ds(pl.multiple_of((1 - d) * PANEL + k * INNER, INNER), INNER)]
        copy = remote(other, theirs.at[rows], dsend.at[k], drecv.at[k], {"depth": 1 - d})
        return copy, pltpu.make_async_copy(mine, s_ref.at[rows], dlocal.at[k])

    for k in range(STEPS):
        for copy in exchange(k):
            copy.start()
    for k in range(STEPS):
        copy, mine = exchange(k)
        mine.wait()
        copy.wait_recv()

        def add(i, carry):
            rows = pl.ds(pl.multiple_of(k * INNER + i * 32, 32), 32)
            s_ref[rows, :] = s_ref[rows, :] + theirs[rows, :]
            return carry

        lax.fori_loop(0, INNER // 32, add, 0)
        launch(k)

    @pl.when(top)
    def _():
        arrive(0)

    ticks(0, EARLY)

    @pl.when(jnp.logical_not(top))
    def _():
        arrive(0)

    other = jnp.logical_not(top)
    plan = [(0, 1, top), (2, 2, top), (6, 3, top), (2, 1, other), (6, 2, other), (10, 3, other)]

    def side(k, i, n):
        tick(n)
        for at, piece_index, who in plan:
            if i == at % TICKS:
                @pl.when((k == at // TICKS) & who)
                def _():
                    arrive(piece_index)

    scratch = (work, inv, held, pivot_block)
    factor_block(diag, inverse.at[0], lower, *scratch, side, EARLY)
    base = EARLY + TICKS * STEPS
    reach = CHUNKS + LAG * max(last, col_groups - 1 - last) + LAG * (row_groups - 1) + 1
    resume = max(base, reach)
    ticks(base, resume)

    def landed(item):
        def step(k, carry):
            finish(*blocks_args(item, k), True)
            return carry

        lax.fori_loop(0, CHUNKS, step, 0)

    landed(0)
    solved[...] = dot(inverse[0], rest[0], 1, 0)
    landed(1)
    whole = theirs.at[:, pl.ds(0, PANEL)]
    whole[...] = rest[1] - dot(solved[...], solved[...], 0, 0)
    for k in range(STEPS):
        settle(k)
        exchange(k)[0].wait_send()

    own_block = r + row_groups * d

    def tiles(count, size, body):
        def step(t, carry):
            body(pl.ds(pl.multiple_of(t * size, size), size), t)
            return carry

        lax.fori_loop(0, count // size, step, 0)

    def live(t, p):
        return t * col_groups + c > p

    def first_rows(lanes, t):
        value = jnp.where(own_block < PANELS, lower[:, lanes], dot(rowp[0], inverse[0, lanes, :], 1, 1))
        crow[0, :, lanes] = value
        left[:, lanes] = jnp.where(own_block > 0, value, 0.0)

    def first_cols(lanes, t):
        value = jnp.where(live(t, 0), dot(inverse[0], colp[0, :, lanes], 1, 0), 0.0)
        ccols[:, lanes] = value
        s_ref[:, lanes] = s_ref[:, lanes] - dot(left[...], value, 1, 0)

    def between_rows(lanes, t):
        rowp[1, :, lanes] = rowp[1, :, lanes] - dot(left[...], solved[:, lanes], 1, 0)

    def second_rows(lanes, t):
        value = jnp.where(own_block > 0, dot(rowp[1], inverse[1, lanes, :], 1, 1), 0.0)
        crow[1, :, lanes] = value
        left[:, lanes] = jnp.where(own_block > 1, value, 0.0)

    def second_cols(lanes, t):
        value = colp[1, :, lanes] - dot(solved[...], ccols[:, lanes], 0, 0)
        value = dot(inverse[1], value, 1, 0)
        value = jnp.where(live(t, 1), value, 0.0)
        s_ref[:, lanes] = s_ref[:, lanes] - dot(left[...], value, 1, 0)

    def arrived_cols(p):
        def step(k, carry):
            finish(*cols_args(p, k), True)
            return carry

        lax.fori_loop(0, CHUNKS, step, 0)

    def give(p):
        sent = crow.at[p, :, pl.ds(pl.multiple_of((1 - d) * half, half), half)]
        there = factor.at[p, pl.ds(pl.multiple_of(d * PANEL, PANEL), PANEL), :]
        return remote(sent, there, fsend.at[p], frecv.at[p], {"depth": 1 - d})

    def keep(p):
        kept = crow[p, :, pl.ds(pl.multiple_of(d * half, half), half)]
        factor[p, pl.ds(pl.multiple_of(d * PANEL, PANEL), PANEL), :] = kept

    def first_panel():
        @pl.when((r == 1) & (d == 0))
        def _():
            lower[...] = solved[...].T

        tiles(PANEL, half, first_rows)
        arrived_cols(0)
        tiles(s_ref.shape[1], PANEL, first_cols)
        keep(0)
        give(0).start()

    lines = 2 * PANELS * CHUNKS + SLACK * max(col_groups - 1, last)
    rings = PANELS * CHUNKS + START + 1 + SLACK * (row_groups - 1)
    ready = max(lines - CHUNKS * PANELS, rings - CHUNKS, 2 * CHUNKS * PANELS)
    early = -(-(ready - resume) // TICKS) - 1
    extra = (early, first_panel) if early < STEPS else None
    factor_block(whole, inverse.at[1], None, *scratch, lambda k, i, n: tick(n), resume, extra)
    ticks(resume + TICKS * STEPS, max(lines, rings))
    if extra is None:
        first_panel()

    def close(k, carry):
        for p in range(PANELS):
            begin, stride, up, down, needed = line_set(p)
            for way, on in ((1, up), (-1, down)):
                @pl.when(on & needed)
                def _():
                    line(p, k, way).wait_send()
            finish(*blocks_args(p, k), False)
            finish(*cols_args(p, k), False)
        return carry

    lax.fori_loop(0, CHUNKS, close, 0)
    arrived_cols(1)
    tiles(PANEL, half, between_rows)
    tiles(PANEL, half, second_rows)
    keep(1)
    give(1).start()
    tiles(s_ref.shape[1], PANEL, second_cols)
    for p in range(PANELS):
        give(p).wait()


def lead(layer, row_groups, col_groups):
    cols = layer.shape[2]
    dma = pltpu.SemaphoreType.DMA
    vmem = pl.BlockSpec(memory_space=pltpu.VMEM)
    f32 = lambda *shape: jax.ShapeDtypeStruct(shape, jnp.float32)
    buffer = lambda *shape: pltpu.VMEM(shape, jnp.float32)
    return pl.pallas_call(
        functools.partial(lead_kernel, (row_groups, col_groups)),
        out_shape=(
            f32(PANEL, cols),
            f32(PANELS, 2 * PANEL, PANEL // 2),
        ),
        in_specs=[pl.BlockSpec(memory_space=pl.ANY)],
        out_specs=(vmem,) * 2,
        scratch_shapes=[
            buffer(PANEL, PANEL),
            buffer(PANEL, cols),
            buffer(PANELS, PANEL, PANEL),
            buffer(PANELS, PANEL, cols),
            buffer(PANELS, PANEL, PANEL),
            buffer(PANEL, PANEL),
            buffer(PANEL, PANEL),
            buffer(PANELS, PANEL, PANEL),
            buffer(PANEL, cols),
            buffer(PANEL, PANEL),
            buffer(PANELS, PANEL, PANEL),
            buffer(INNER, INNER),
            buffer(INNER, INNER),
            buffer(INNER, PANEL),
            buffer(INNER, INNER),
            dma((STEPS,)),
            dma((STEPS,)),
            dma((STEPS,)),
            dma((STEPS, row_groups + col_groups - 1)),
            dma((STEPS,)),
            dma((PANELS, CHUNKS, 2)),
            dma((PANELS, CHUNKS)),
        ]
        + 2 * [dma((PANELS, CHUNKS)), dma((PANELS, CHUNKS)), dma((PANELS, 2, CHUNKS)), dma((PANELS, 2, CHUNKS))]
        + [dma((PANELS,)), dma((PANELS,)), dma],
        compiler_params=pltpu.CompilerParams(has_side_effects=True, vmem_limit_bytes=60 * 1024 * 1024),
        name="lead",
    )(layer)


def per_device(layers):
    row_groups = lax.axis_size("row")
    col_groups = lax.axis_size("col")
    depth_groups = lax.axis_size("depth")
    assert layers.shape[1] == PANEL * depth_groups and depth_groups == 2
    assert PANELS == 2 and row_groups >= PANELS and col_groups >= PANELS

    schur, factor = lead(layers, row_groups, col_groups)
    return factor, schur


def solution(mesh):
    return jax.shard_map(
        per_device,
        mesh=mesh,
        in_specs=(P("depth", "row", "col"),),
        out_specs=(P(None, "row", "depth"), P(("row", "depth"), "col")),
        check_vma=False,
    )
```
